8 devices in a mesh: dp: 2 (over z, y), tp: 4 (over x, core).
Axes of the slice: x: 2, y: 2, z: 1, core: 2. Of those that a mesh axis runs over, the one named last changes fastest.
Arguments:
- hidden_in: bfloat16 [2048, 2048], P(('dp', 'tp')), parts along dimension 0
- k_cache: bfloat16 [2048, 512, 256], P(('dp', 'tp')), parts along dimension 0
- v_cache: bfloat16 [2048, 512, 256], P(('dp', 'tp')), parts along dimension 0
- cache_len: int32 [2048], P(('dp', 'tp')), parts along dimension 0
- norm_attn: bfloat16 [2048], replicated
- norm_mlp: bfloat16 [2048], replicated
- w_q: bfloat16 [2048, 2048], replicated
- w_k: bfloat16 [2048, 256], replicated
- w_v: bfloat16 [2048, 256], replicated
- w_o: bfloat16 [2048, 2048], replicated
- w_gate: bfloat16 [2048, 16384], P(None, 'tp')
- w_up: bfloat16 [2048, 16384], P(None, 'tp')
- w_down: bfloat16 [16384, 2048], P('tp')
Outputs:
- output 1: bfloat16 [2048, 2048], P(('dp', 'tp')), parts along dimension 0
- output 2: bfloat16 [2048, 256], P(('dp', 'tp')), parts along dimension 0
- output 3: bfloat16 [2048, 256], P(('dp', 'tp')), parts along dimension 0
There are 2 independent parts. The reference program is written for one: setup_inputs(seed, part) draws one part's arguments, and reference() takes and returns one part's arrays. A program takes and returns all parts, laid end to end along the dimension named above; an argument that names none is the same for every part.
All inputs are finite; a program needn't handle non-finite values.
Results may differ from the reference program's by a relative error of at most 0.00565983.
Values are sent between devices in bfloat16 or wider.
A program may use at most 1 GiB of HBM per device.

```python
import jax
import jax.numpy as jnp
from jax import lax

D_MODEL = 2048
NUM_HEADS = 8
HEAD_DIM = 256
FF_DIM = 16384
BATCH_ROWS = 1024
CACHE_SIZE = 512


def scaled_normal(key_w, shape_w, fan_in):
    return (jax.random.normal(key_w, shape_w, jnp.float32) * fan_in ** -0.5).astype(jnp.bfloat16)


def setup_inputs(seed: int = 0, part: int = 0) -> dict:
    base_key = jax.random.key(seed)
    shared_keys = jax.random.split(base_key, 9)
    own_keys = jax.random.split(jax.random.fold_in(base_key, part), 5)
    q_width = NUM_HEADS * HEAD_DIM
    hidden_in = jax.random.normal(own_keys[0], (BATCH_ROWS, D_MODEL), jnp.float32)
    k_cache = 2.0 * jax.random.normal(own_keys[1], (BATCH_ROWS, CACHE_SIZE, HEAD_DIM), jnp.float32)
    v_mean = 0.7 * jax.random.normal(own_keys[2], (BATCH_ROWS, 1, HEAD_DIM), jnp.float32)
    v_cache = v_mean + jax.random.normal(own_keys[3], (BATCH_ROWS, CACHE_SIZE, HEAD_DIM), jnp.float32)
    cache_len = jax.random.randint(own_keys[4], (BATCH_ROWS,), 0, CACHE_SIZE, jnp.int32)
    cache_len = cache_len.at[0].set(CACHE_SIZE - 1)
    return {
        'hidden_in': hidden_in.astype(jnp.bfloat16),
        'k_cache': k_cache.astype(jnp.bfloat16),
        'v_cache': v_cache.astype(jnp.bfloat16),
        'cache_len': cache_len,
        'norm_attn': (0.3 * jax.random.normal(shared_keys[0], (D_MODEL,), jnp.float32)).astype(jnp.bfloat16),
        'norm_mlp': (0.3 * jax.random.normal(shared_keys[1], (D_MODEL,), jnp.float32)).astype(jnp.bfloat16),
        'w_q': scaled_normal(shared_keys[2], (D_MODEL, q_width), D_MODEL),
        'w_k': scaled_normal(shared_keys[3], (D_MODEL, HEAD_DIM), D_MODEL),
        'w_v': scaled_normal(shared_keys[4], (D_MODEL, HEAD_DIM), D_MODEL),
        'w_o': scaled_normal(shared_keys[5], (q_width, D_MODEL), q_width),
        'w_gate': scaled_normal(shared_keys[6], (D_MODEL, FF_DIM), D_MODEL),
        'w_up': scaled_normal(shared_keys[7], (D_MODEL, FF_DIM), D_MODEL),
        'w_down': scaled_normal(shared_keys[8], (FF_DIM, D_MODEL), FF_DIM),
    }


def rms_scale(values, gain_vec):
    wide_vals = values.astype(jnp.float32)
    inv_rms = lax.rsqrt(jnp.mean(wide_vals * wide_vals, axis=-1, keepdims=True) + 1e-6)
    return (wide_vals * inv_rms * (1.0 + gain_vec.astype(jnp.float32))).astype(jnp.bfloat16)


def rope_tables(positions, head_dim):
    half_dim = head_dim // 2
    inv_freq = 10000.0 ** (-2.0 * jnp.arange(half_dim, dtype=jnp.float32) / head_dim)
    angles = positions.astype(jnp.float32)[:, None] * inv_freq[None, :]
    return jnp.cos(angles), jnp.sin(angles)


def rotary(values, cos_t, sin_t):
    half_dim = values.shape[-1] // 2
    first_half = values[..., :half_dim]
    second_half = values[..., half_dim:]
    return jnp.concatenate([first_half * cos_t - second_half * sin_t, second_half * cos_t + first_half * sin_t], axis=-1)


def attend_row(row_args):
    q_row, k_row, v_row, k_hist, v_hist, position = row_args
    q_wide = q_row.astype(jnp.float32)
    hist_score = jnp.einsum('hd,td->ht', q_wide, k_hist.astype(jnp.float32))
    new_score = jnp.einsum('hd,d->h', q_wide, k_row.astype(jnp.float32))
    valid_mask = jnp.arange(k_hist.shape[0]) < position
    hist_score = jnp.where(valid_mask[None, :], hist_score, -jnp.inf)
    peak_score = jnp.maximum(jnp.max(hist_score, axis=-1), new_score)
    hist_weight = jnp.exp(hist_score - peak_score[:, None])
    new_weight = jnp.exp(new_score - peak_score)
    weight_sum = jnp.sum(hist_weight, axis=-1) + new_weight
    hist_prob = (hist_weight / weight_sum[:, None]).astype(jnp.bfloat16)
    new_prob = (new_weight / weight_sum).astype(jnp.bfloat16)
    attn_out = jnp.einsum('ht,td->hd', hist_prob.astype(jnp.float32), v_hist.astype(jnp.float32))
    attn_out = attn_out + new_prob.astype(jnp.float32)[:, None] * v_row.astype(jnp.float32)[None, :]
    return attn_out.astype(jnp.bfloat16)


def reference(hidden_in, k_cache, v_cache, cache_len, norm_attn, norm_mlp, w_q, w_k, w_v, w_o, w_gate, w_up, w_down):
    num_rows = hidden_in.shape[0]
    normed = rms_scale(hidden_in, norm_attn)
    q_lin = jnp.dot(normed, w_q, preferred_element_type=jnp.float32).reshape(num_rows, NUM_HEADS, HEAD_DIM)
    k_lin = jnp.dot(normed, w_k, preferred_element_type=jnp.float32)
    v_new = jnp.dot(normed, w_v, preferred_element_type=jnp.float32).astype(jnp.bfloat16)
    cos_t, sin_t = rope_tables(cache_len, HEAD_DIM)
    q_rot = (rotary(q_lin, cos_t[:, None, :], sin_t[:, None, :]) * HEAD_DIM ** -0.5).astype(jnp.bfloat16)
    k_new = rotary(k_lin, cos_t, sin_t).astype(jnp.bfloat16)
    attn_out = lax.map(attend_row, (q_rot, k_new, v_new, k_cache, v_cache, cache_len))
    mixed = jnp.dot(attn_out.reshape(num_rows, NUM_HEADS * HEAD_DIM), w_o, preferred_element_type=jnp.float32)
    x_mid = hidden_in.astype(jnp.float32) + mixed
    xn_mid = rms_scale(x_mid, norm_mlp)
    gate_act = jnp.dot(xn_mid, w_gate, preferred_element_type=jnp.float32)
    up_act = jnp.dot(xn_mid, w_up, preferred_element_type=jnp.float32)
    hidden_act = (jax.nn.gelu(gate_act, approximate=True) * up_act).astype(jnp.bfloat16)
    down_sum = jnp.dot(hidden_act, w_down, preferred_element_type=jnp.float32)
    hidden_out = (x_mid + down_sum).astype(jnp.bfloat16)
    return hidden_out, k_new, v_new
```

```python
import functools

import jax
import jax.numpy as jnp
from jax import lax
from jax.experimental import pallas as pl
from jax.experimental.pallas import tpu as pltpu
from jax.sharding import PartitionSpec as P

GROUP = 8
RING = 4
GRAIN = 16


def rms_scale(values, gain_vec):
    wide_vals = values.astype(jnp.float32)
    inv_rms = lax.rsqrt(jnp.mean(wide_vals * wide_vals, axis=-1, keepdims=True) + 1e-6)
    return (wide_vals * inv_rms * (1.0 + gain_vec.astype(jnp.float32))).astype(jnp.bfloat16)


def rope_tables(positions, head_dim):
    half_dim = head_dim // 2
    inv_freq = 10000.0 ** (-2.0 * jnp.arange(half_dim, dtype=jnp.float32) / head_dim)
    angles = positions.astype(jnp.float32)[:, None] * inv_freq[None, :]
    return jnp.cos(angles), jnp.sin(angles)


def rotary(values, cos_t, sin_t):
    half_dim = values.shape[-1] // 2
    first_half = values[..., :half_dim]
    second_half = values[..., half_dim:]
    return jnp.concatenate([first_half * cos_t - second_half * sin_t, second_half * cos_t + first_half * sin_t], axis=-1)


def attend_kernel(num_groups, len_ref, q_ref, kn_ref, vn_ref, k_hbm, v_hbm, o_ref,
                  k_buf, v_buf, s_buf, k_sem, v_sem):
    cap = k_buf.shape[1]

    def copy(src_hbm, dst_buf, sems, group, lane):
        row = group * GROUP + lane
        slot = lax.rem(group, RING) * GROUP + lane
        used = pl.multiple_of((len_ref[row] + (GRAIN - 1)) // GRAIN * GRAIN, GRAIN)
        return pltpu.make_async_copy(src_hbm.at[row, pl.ds(0, used), :],
                                     dst_buf.at[slot, pl.ds(0, used), :], sems.at[slot])

    def start(src_hbm, dst_buf, sems, group):
        for lane in range(GROUP):
            copy(src_hbm, dst_buf, sems, group, lane).start()

    def wait(src_hbm, dst_buf, sems, group):
        for lane in range(GROUP):
            copy(src_hbm, dst_buf, sems, group, lane).wait()

    def scores(group):
        base = lax.rem(group, RING) * GROUP
        for lane in range(GROUP):
            s_buf[lax.rem(group, 2), lane] = lax.dot_general(
                q_ref[group * GROUP + lane], k_buf[base + lane],
                (((1,), (1,)), ((), ())), preferred_element_type=jnp.float32)

    def outputs(group):
        base = lax.rem(group, RING) * GROUP
        first = pl.multiple_of(group * GROUP, GROUP)
        k_new = kn_ref[pl.ds(first, GROUP), :]
        v_new = vn_ref[pl.ds(first, GROUP), :]
        place = lax.broadcasted_iota(jnp.int32, (GROUP, cap), 1)
        for lane in range(GROUP):
            row = first + lane
            score = jnp.where(place < len_ref[row], s_buf[lax.rem(group, 2), lane], -jnp.inf)
            q_wide = q_ref[row].astype(jnp.float32)
            new_score = jnp.sum(q_wide * k_new[lane:lane + 1, :], axis=-1, keepdims=True)
            peak = jnp.maximum(jnp.max(score, axis=-1, keepdims=True), new_score)
            weight = jnp.exp(score - peak)
            new_weight = jnp.exp(new_score - peak)
            scale = 1.0 / (jnp.sum(weight, axis=-1, keepdims=True) + new_weight)
            prob = (weight * scale).astype(jnp.bfloat16)
            new_prob = (new_weight * scale).astype(jnp.bfloat16).astype(jnp.float32)
            mixed = jnp.dot(prob, v_buf[base + lane], preferred_element_type=jnp.float32)
            o_ref[row] = (mixed + new_prob * v_new[lane:lane + 1, :]).astype(jnp.bfloat16)

    for group in range(RING):
        start(k_hbm, k_buf, k_sem, group)

    def clear(slot, carry):
        v_buf[slot] = jnp.zeros(v_buf.shape[1:], v_buf.dtype)
        return carry

    lax.fori_loop(0, v_buf.shape[0], clear, 0)
    for group in range(RING):
        start(v_hbm, v_buf, v_sem, group)

    wait(k_hbm, k_buf, k_sem, 0)
    scores(0)
    start(k_hbm, k_buf, k_sem, RING)

    def step(group, carry):
        wait(k_hbm, k_buf, k_sem, group + 1)
        wait(v_hbm, v_buf, v_sem, group)
        scores(group + 1)
        outputs(group)

        @pl.when(group + 1 + RING < num_groups)
        def _():
            start(k_hbm, k_buf, k_sem, group + 1 + RING)

        @pl.when(group + RING < num_groups)
        def _():
            start(v_hbm, v_buf, v_sem, group + RING)
        return carry

    lax.fori_loop(0, num_groups - 1, step, 0)
    wait(v_hbm, v_buf, v_sem, num_groups - 1)
    outputs(num_groups - 1)


def attend(q_rot, k_new, v_new, k_cache, v_cache, cache_len):
    rows, heads, dim = q_rot.shape
    cap = k_cache.shape[1]
    vmem = pl.BlockSpec(memory_space=pltpu.VMEM)
    hbm = pl.BlockSpec(memory_space=pl.ANY)
    return pl.pallas_call(
        functools.partial(attend_kernel, rows // GROUP),
        name='attend',
        out_shape=jax.ShapeDtypeStruct((rows, heads, dim), jnp.bfloat16),
        in_specs=[pl.BlockSpec(memory_space=pltpu.SMEM), vmem, vmem, vmem, hbm, hbm],
        out_specs=vmem,
        scratch_shapes=[
            pltpu.VMEM((RING * GROUP, cap, dim), jnp.bfloat16),
            pltpu.VMEM((RING * GROUP, cap, dim), jnp.bfloat16),
            pltpu.VMEM((2, GROUP, heads, cap), jnp.float32),
            pltpu.SemaphoreType.DMA((RING * GROUP,)),
            pltpu.SemaphoreType.DMA((RING * GROUP,)),
        ],
        compiler_params=pltpu.CompilerParams(vmem_limit_bytes=40 * 1024 * 1024),
        cost_estimate=pl.CostEstimate(flops=4 * rows * heads * dim * cap,
                                      bytes_accessed=2 * rows * cap * dim * 2,
                                      transcendentals=rows * heads * cap),
    )(cache_len, q_rot, k_new.astype(jnp.float32), v_new.astype(jnp.float32), k_cache, v_cache)


def attention_block(hidden_in, k_cache, v_cache, cache_len, norm_attn, w_q, w_k, w_v, w_o):
    num_rows = hidden_in.shape[0]
    head_dim = w_k.shape[1]
    num_heads = w_q.shape[1] // head_dim
    normed = rms_scale(hidden_in, norm_attn)
    q_lin = jnp.dot(normed, w_q, preferred_element_type=jnp.float32).reshape(num_rows, num_heads, head_dim)
    k_lin = jnp.dot(normed, w_k, preferred_element_type=jnp.float32)
    v_new = jnp.dot(normed, w_v, preferred_element_type=jnp.float32).astype(jnp.bfloat16)
    cos_t, sin_t = rope_tables(cache_len, head_dim)
    q_rot = (rotary(q_lin, cos_t[:, None, :], sin_t[:, None, :]) * head_dim ** -0.5).astype(jnp.bfloat16)
    k_new = rotary(k_lin, cos_t, sin_t).astype(jnp.bfloat16)
    attn_out = attend(q_rot, k_new, v_new, k_cache, v_cache, cache_len)
    mixed = jnp.dot(attn_out.reshape(num_rows, num_heads * head_dim), w_o, preferred_element_type=jnp.float32)
    return hidden_in.astype(jnp.float32) + mixed, k_new, v_new


def solution(mesh):
    row_spec = P(('dp', 'tp'), None)
    cache_spec = P(('dp', 'tp'), None, None)
    full_vec = P(None)
    full_mat = P(None, None)

    def per_device(hidden_in, k_cache, v_cache, cache_len, norm_attn, norm_mlp, w_q, w_k, w_v, w_o, w_gate, w_up, w_down):
        x_mid, k_new, v_new = attention_block(hidden_in, k_cache, v_cache, cache_len, norm_attn, w_q, w_k, w_v, w_o)
        xn_mid = rms_scale(x_mid, norm_mlp)
        group_rows = lax.all_gather(xn_mid, 'tp', axis=0, tiled=True)
        gate_act = jnp.dot(group_rows, w_gate, preferred_element_type=jnp.float32)
        up_act = jnp.dot(group_rows, w_up, preferred_element_type=jnp.float32)
        hidden_act = (jax.nn.gelu(gate_act, approximate=True) * up_act).astype(jnp.bfloat16)
        part_sum = jnp.dot(hidden_act, w_down, preferred_element_type=jnp.float32)
        down_sum = lax.psum_scatter(part_sum, 'tp', scatter_dimension=0, tiled=True)
        return (x_mid + down_sum).astype(jnp.bfloat16), k_new, v_new

    return jax.shard_map(
        per_device,
        mesh=mesh,
        in_specs=(row_spec, cache_spec, cache_spec, P(('dp', 'tp')), full_vec, full_vec,
                  full_mat, full_mat, full_mat, full_mat, P(None, 'tp'), P(None, 'tp'), P('tp', None)),
        out_specs=(row_spec, row_spec, row_spec),
        check_vma=False,
    )
```

```python
import functools

import jax
import jax.numpy as jnp
from jax import lax
from jax.experimental import pallas as pl
from jax.experimental.pallas import tpu as pltpu
from jax.sharding import PartitionSpec as P

GROUP = 8
RING = 4
GRAIN = 16


def rms_scale(values, gain_vec):
    wide_vals = values.astype(jnp.float32)
    inv_rms = lax.rsqrt(jnp.mean(wide_vals * wide_vals, axis=-1, keepdims=True) + 1e-6)
    return (wide_vals * inv_rms * (1.0 + gain_vec.astype(jnp.float32))).astype(jnp.bfloat16)


def rope_tables(positions, head_dim):
    half_dim = head_dim // 2
    inv_freq = 10000.0 ** (-2.0 * jnp.arange(half_dim, dtype=jnp.float32) / head_dim)
    angles = positions.astype(jnp.float32)[:, None] * inv_freq[None, :]
    return jnp.cos(angles), jnp.sin(angles)


def rotary(values, cos_t, sin_t):
    half_dim = values.shape[-1] // 2
    first_half = values[..., :half_dim]
    second_half = values[..., half_dim:]
    return jnp.concatenate([first_half * cos_t - second_half * sin_t, second_half * cos_t + first_half * sin_t], axis=-1)


def attend_kernel(num_groups, len_ref, q_ref, kn_ref, vn_ref, k_hbm, v_hbm, o_ref,
                  k_buf, v_buf, s_buf, k_sem, v_sem):
    cap = k_buf.shape[1]

    def copy(src_hbm, dst_buf, sems, group, lane):
        row = group * GROUP + lane
        slot = lax.rem(group, RING) * GROUP + lane
        used = pl.multiple_of((len_ref[row] + (GRAIN - 1)) // GRAIN * GRAIN, GRAIN)
        return pltpu.make_async_copy(src_hbm.at[row, pl.ds(0, used), :],
                                     dst_buf.at[slot, pl.ds(0, used), :], sems.at[slot])

    def start(src_hbm, dst_buf, sems, group):
        for lane in range(GROUP):
            copy(src_hbm, dst_buf, sems, group, lane).start()

    def wait(src_hbm, dst_buf, sems, group):
        for lane in range(GROUP):
            copy(src_hbm, dst_buf, sems, group, lane).wait()

    def scores(group):
        base = lax.rem(group, RING) * GROUP
        for lane in range(GROUP):
            s_buf[lax.rem(group, 2), lane] = lax.dot_general(
                q_ref[group * GROUP + lane], k_buf[base + lane],
                (((1,), (1,)), ((), ())), preferred_element_type=jnp.float32)

    def outputs(group):
        base = lax.rem(group, RING) * GROUP
        first = pl.multiple_of(group * GROUP, GROUP)
        k_new = kn_ref[pl.ds(first, GROUP), :]
        v_new = vn_ref[pl.ds(first, GROUP), :]
        place = lax.broadcasted_iota(jnp.int32, (GROUP, cap), 1)
        for lane in range(GROUP):
            row = first + lane
            score = jnp.where(place < len_ref[row], s_buf[lax.rem(group, 2), lane], -jnp.inf)
            q_wide = q_ref[row].astype(jnp.float32)
            new_score = jnp.sum(q_wide * k_new[lane:lane + 1, :], axis=-1, keepdims=True)
            peak = jnp.maximum(jnp.max(score, axis=-1, keepdims=True), new_score)
            weight = jnp.exp(score - peak)
            new_weight = jnp.exp(new_score - peak)
            scale = 1.0 / (jnp.sum(weight, axis=-1, keepdims=True) + new_weight)
            prob = (weight * scale).astype(jnp.bfloat16)
            new_prob = (new_weight * scale).astype(jnp.bfloat16).astype(jnp.float32)
            mixed = jnp.dot(prob, v_buf[base + lane], preferred_element_type=jnp.float32)
            o_ref[row] = (mixed + new_prob * v_new[lane:lane + 1, :]).astype(jnp.bfloat16)

    for group in range(RING):
        start(k_hbm, k_buf, k_sem, group)

    def clear(slot, carry):
        v_buf[slot] = jnp.zeros(v_buf.shape[1:], v_buf.dtype)
        return carry

    lax.fori_loop(0, v_buf.shape[0], clear, 0)
    for group in range(RING):
        start(v_hbm, v_buf, v_sem, group)

    wait(k_hbm, k_buf, k_sem, 0)
    scores(0)
    start(k_hbm, k_buf, k_sem, RING)

    def step(group, carry):
        wait(k_hbm, k_buf, k_sem, group + 1)
        wait(v_hbm, v_buf, v_sem, group)
        scores(group + 1)
        outputs(group)

        @pl.when(group + 1 + RING < num_groups)
        def _():
            start(k_hbm, k_buf, k_sem, group + 1 + RING)

        @pl.when(group + RING < num_groups)
        def _():
            start(v_hbm, v_buf, v_sem, group + RING)
        return carry

    lax.fori_loop(0, num_groups - 1, step, 0)
    wait(v_hbm, v_buf, v_sem, num_groups - 1)
    outputs(num_groups - 1)


def attend(q_rot, k_new, v_new, k_cache, v_cache, cache_len):
    rows, heads, dim = q_rot.shape
    cap = k_cache.shape[1]
    vmem = pl.BlockSpec(memory_space=pltpu.VMEM)
    hbm = pl.BlockSpec(memory_space=pl.ANY)
    return pl.pallas_call(
        functools.partial(attend_kernel, rows // GROUP),
        name='attend',
        out_shape=jax.ShapeDtypeStruct((rows, heads, dim), jnp.bfloat16),
        in_specs=[pl.BlockSpec(memory_space=pltpu.SMEM), vmem, vmem, vmem, hbm, hbm],
        out_specs=vmem,
        scratch_shapes=[
            pltpu.VMEM((RING * GROUP, cap, dim), jnp.bfloat16),
            pltpu.VMEM((RING * GROUP, cap, dim), jnp.bfloat16),
            pltpu.VMEM((2, GROUP, heads, cap), jnp.float32),
            pltpu.SemaphoreType.DMA((RING * GROUP,)),
            pltpu.SemaphoreType.DMA((RING * GROUP,)),
        ],
        compiler_params=pltpu.CompilerParams(vmem_limit_bytes=40 * 1024 * 1024),
        cost_estimate=pl.CostEstimate(flops=4 * rows * heads * dim * cap,
                                      bytes_accessed=2 * rows * cap * dim * 2,
                                      transcendentals=rows * heads * cap),
    )(cache_len, q_rot, k_new.astype(jnp.float32), v_new.astype(jnp.float32), k_cache, v_cache)


def attention_block(hidden_in, k_cache, v_cache, cache_len, norm_attn, w_q, w_k, w_v, w_o):
    num_rows = hidden_in.shape[0]
    head_dim = w_k.shape[1]
    num_heads = w_q.shape[1] // head_dim
    normed = rms_scale(hidden_in, norm_attn)
    q_lin = jnp.dot(normed, w_q, preferred_element_type=jnp.float32).reshape(num_rows, num_heads, head_dim)
    k_lin = jnp.dot(normed, w_k, preferred_element_type=jnp.float32)
    v_new = jnp.dot(normed, w_v, preferred_element_type=jnp.float32).astype(jnp.bfloat16)
    cos_t, sin_t = rope_tables(cache_len, head_dim)
    q_rot = (rotary(q_lin, cos_t[:, None, :], sin_t[:, None, :]) * head_dim ** -0.5).astype(jnp.bfloat16)
    k_new = rotary(k_lin, cos_t, sin_t).astype(jnp.bfloat16)
    attn_out = attend(q_rot, k_new, v_new, k_cache, v_cache, cache_len)
    mixed = jnp.dot(attn_out.reshape(num_rows, num_heads * head_dim), w_o, preferred_element_type=jnp.float32)
    return hidden_in.astype(jnp.float32) + mixed, k_new, v_new


HID_BLOCK = 512
OUT_BLOCK = 512
WEIGHT_RING = 3
MESH = pl.DeviceIdType.MESH


def mlp_kernel(xn_ref, xmid_ref, wg_hbm, wu_hbm, wd_hbm, out_ref,
               x_all, h_buf, g_buf, u_buf, wg_buf, wu_buf, wd_buf, acc_buf,
               d_send, d_recv, c_send, c_recv, p_send, p_recv,
               w_sem, wd_sem, send_sem, recv_sem):
    rows, width = xn_ref.shape
    half = rows // 2
    hidden = wg_hbm.shape[1]
    num_hid = hidden // HID_BLOCK
    num_out = width // OUT_BLOCK
    num_steps = 4 * num_hid
    me = lax.axis_index('tp')
    partner = me + 1 - 2 * lax.rem(me, 2)
    counter = lax.rem(me + 2, 4)

    barrier = pltpu.get_barrier_semaphore()
    for peer in (partner, counter):
        pl.semaphore_signal(barrier, inc=1, device_id={'tp': peer}, device_id_type=MESH)

    def weight_copies(step):
        slot = lax.rem(step, WEIGHT_RING)
        cols = pl.ds(pl.multiple_of(lax.rem(step, num_hid) * HID_BLOCK, HID_BLOCK), HID_BLOCK)
        return (pltpu.make_async_copy(wg_hbm.at[:, cols], wg_buf.at[slot], w_sem.at[slot, 0]),
                pltpu.make_async_copy(wu_hbm.at[:, cols], wu_buf.at[slot], w_sem.at[slot, 1]))

    def down_copy(block):
        return pltpu.make_async_copy(wd_hbm.at[:, pl.ds(block * OUT_BLOCK, OUT_BLOCK)],
                                     wd_buf.at[block], wd_sem.at[block])

    def remote(src, dst, index, peer):
        return pltpu.make_async_remote_copy(
            src_ref=src, dst_ref=dst, send_sem=send_sem.at[index], recv_sem=recv_sem.at[index],
            device_id={'tp': peer}, device_id_type=MESH)

    gather_partner = remote(xn_ref, x_all.at[0], 0, partner)
    gather_counter = [remote(xn_ref.at[pl.ds(i * half, half), :], x_all.at[1 + i, pl.ds(0, half), :], 1 + i, counter)
                      for i in range(2)]
    forward = [remote(x_all.at[1 + i, pl.ds(0, half), :], x_all.at[1 + i, pl.ds(half, half), :], 3 + i, partner)
               for i in range(2)]

    def cross(i, n):
        return remote(d_send.at[i, n], d_recv.at[i, n], 5 + i * num_out + n, partner)

    def home(i, n):
        return remote(c_send.at[i, n], c_recv.at[i, n], 5 + (2 + i) * num_out + n, counter)

    def side(n):
        return remote(p_send.at[n], p_recv.at[n], 5 + 4 * num_out + n, partner)

    for step in range(WEIGHT_RING):
        for copy in weight_copies(step):
            copy.start()
    for block in range(num_out):
        down_copy(block).start()
    pl.semaphore_wait(barrier, 2)
    gather_partner.start()
    for copy in gather_counter:
        copy.start()

    def hidden_dots(x_ref, step):
        slot = lax.rem(step, WEIGHT_RING)
        keep = lax.rem(step, 2)
        g_buf[keep] = jnp.dot(x_ref[...], wg_buf[slot], preferred_element_type=jnp.float32)
        u_buf[keep] = jnp.dot(x_ref[...], wu_buf[slot], preferred_element_type=jnp.float32)

    def activate(step, block):
        keep = lax.rem(step, 2)
        cols = pl.ds(pl.multiple_of(block * HID_BLOCK, HID_BLOCK), HID_BLOCK)
        h_buf[:, cols] = (jax.nn.gelu(g_buf[keep], approximate=True) * u_buf[keep]).astype(jnp.bfloat16)

    def prefetch(step):
        @pl.when(step + WEIGHT_RING < num_steps)
        def _():
            for copy in weight_copies(step + WEIGHT_RING):
                copy.start()

    def hidden_phase(number, x_ref):
        first = number * num_hid
        for copy in weight_copies(first):
            copy.wait()
        hidden_dots(x_ref, first)
        prefetch(first)

        def body(block, carry):
            step = first + block
            for copy in weight_copies(step):
                copy.wait()
            hidden_dots(x_ref, step)
            activate(step - 1, block - 1)
            prefetch(step)
            return carry

        lax.fori_loop(1, num_hid, body, 0)
        activate(first + num_hid - 1, num_hid - 1)

    def down(n):
        return jnp.dot(h_buf[...], wd_buf[n], preferred_element_type=jnp.float32)

    gather_partner.wait_recv()
    hidden_phase(0, x_all.at[0])
    for n in range(num_out):
        down_copy(n).wait()
        p_send[n] = down(n)
        side(n).start()
    gather_counter[0].wait_recv()
    forward[0].start()

    for i in range(2):
        forward[i].wait_recv()
        hidden_phase(1 + i, x_all.at[1 + i])
        if i == 0:
            gather_counter[1].wait_recv()
            forward[1].start()

        def finish(n, i=i):
            cross(i, n).wait_recv()
            c_send[i, n] = c_send[i, n] + d_recv[i, n]
            home(i, n).start()

        def body(n, carry, i=i):
            part = down(n)
            c_send[i, n] = part[:half]
            d_send[i, n] = part[half:]
            cross(i, n).start()

            @pl.when(n > 0)
            def _():
                finish(n - 1)
            return carry

        lax.fori_loop(0, num_out, body, 0)
        finish(num_out - 1)

    hidden_phase(3, xn_ref)

    def own(n, carry):
        acc_buf[n] = down(n)
        return carry

    lax.fori_loop(0, num_out, own, 0)

    def settle(n, carry):
        cols = pl.ds(pl.multiple_of(n * OUT_BLOCK, OUT_BLOCK), OUT_BLOCK)
        side(n).wait_recv()
        for i in range(2):
            part = pl.ds(i * half, half)
            home(i, n).wait_recv()
            total = acc_buf[n, part, :] + p_recv[n, part, :] + c_recv[i, n]
            out_ref[part, cols] = (xmid_ref[part, cols] + total).astype(jnp.bfloat16)
        return carry

    lax.fori_loop(0, num_out, settle, 0)

    gather_partner.wait_send()
    for i in range(2):
        gather_counter[i].wait_send()
        forward[i].wait_send()

    def drain(n, carry):
        side(n).wait_send()
        for i in range(2):
            cross(i, n).wait_send()
            home(i, n).wait_send()
        return carry

    lax.fori_loop(0, num_out, drain, 0)


def mlp_block(xn_mid, x_mid, w_gate, w_up, w_down):
    rows, width = xn_mid.shape
    half = rows // 2
    hidden = w_gate.shape[1]
    num_out = width // OUT_BLOCK
    num_copies = 5 + 5 * num_out
    vmem = pl.BlockSpec(memory_space=pltpu.VMEM)
    hbm = pl.BlockSpec(memory_space=pl.ANY)
    return pl.pallas_call(
        mlp_kernel,
        name='mlp',
        out_shape=jax.ShapeDtypeStruct((rows, width), jnp.bfloat16),
        in_specs=[vmem, vmem, hbm, hbm, hbm],
        out_specs=vmem,
        scratch_shapes=[
            pltpu.VMEM((3, rows, width), jnp.bfloat16),
            pltpu.VMEM((rows, hidden), jnp.bfloat16),
            pltpu.VMEM((2, rows, HID_BLOCK), jnp.float32),
            pltpu.VMEM((2, rows, HID_BLOCK), jnp.float32),
            pltpu.VMEM((WEIGHT_RING, width, HID_BLOCK), jnp.bfloat16),
            pltpu.VMEM((WEIGHT_RING, width, HID_BLOCK), jnp.bfloat16),
            pltpu.VMEM((num_out, hidden, OUT_BLOCK), jnp.bfloat16),
            pltpu.VMEM((num_out, rows, OUT_BLOCK), jnp.float32),
            pltpu.VMEM((2, num_out, half, OUT_BLOCK), jnp.float32),
            pltpu.VMEM((2, num_out, half, OUT_BLOCK), jnp.float32),
            pltpu.VMEM((2, num_out, half, OUT_BLOCK), jnp.float32),
            pltpu.VMEM((2, num_out, half, OUT_BLOCK), jnp.float32),
            pltpu.VMEM((num_out, rows, OUT_BLOCK), jnp.float32),
            pltpu.VMEM((num_out, rows, OUT_BLOCK), jnp.float32),
            pltpu.SemaphoreType.DMA((WEIGHT_RING, 2)),
            pltpu.SemaphoreType.DMA((num_out,)),
            pltpu.SemaphoreType.DMA((num_copies,)),
            pltpu.SemaphoreType.DMA((num_copies,)),
        ],
        compiler_params=pltpu.CompilerParams(collective_id=0, has_side_effects=True,
                                             vmem_limit_bytes=62 * 1024 * 1024),
        cost_estimate=pl.CostEstimate(flops=24 * rows * width * hidden,
                                      bytes_accessed=9 * width * hidden * 2,
                                      transcendentals=4 * rows * hidden),
    )(xn_mid, x_mid, w_gate, w_up, w_down)


def solution(mesh):
    row_spec = P(('dp', 'tp'), None)
    cache_spec = P(('dp', 'tp'), None, None)
    full_vec = P(None)
    full_mat = P(None, None)

    def per_device(hidden_in, k_cache, v_cache, cache_len, norm_attn, norm_mlp, w_q, w_k, w_v, w_o, w_gate, w_up, w_down):
        x_mid, k_new, v_new = attention_block(hidden_in, k_cache, v_cache, cache_len, norm_attn, w_q, w_k, w_v, w_o)
        xn_mid = rms_scale(x_mid, norm_mlp)
        hidden_out = mlp_block(xn_mid, x_mid, w_gate, w_up, w_down)
        return hidden_out, k_new, v_new

    return jax.shard_map(
        per_device,
        mesh=mesh,
        in_specs=(row_spec, cache_spec, cache_spec, P(('dp', 'tp')), full_vec, full_vec,
                  full_mat, full_mat, full_mat, full_mat, P(None, 'tp'), P(None, 'tp'), P('tp', None)),
        out_specs=(row_spec, row_spec, row_spec),
        check_vma=False,
    )
```

```python
import functools

import jax
import jax.numpy as jnp
from jax import lax
from jax.experimental import pallas as pl
from jax.experimental.pallas import tpu as pltpu
from jax.sharding import PartitionSpec as P

GROUP = 16
RING = 3
GRAIN = 16
TILE = 128
PROJ_BLOCK = 512
NORM_ROWS = 32
LANES = 128
PARTS = 2


def rms_scale(values, gain_ref, store):
    wide_vals = values.astype(jnp.float32)
    inv_rms = lax.rsqrt(jnp.mean(wide_vals * wide_vals, axis=-1, keepdims=True) + 1e-6)
    gain = 1.0 + gain_ref[...].astype(jnp.float32)
    for i in range(gain.shape[0]):
        cols = slice(i * LANES, (i + 1) * LANES)
        store(cols, (wide_vals[:, cols] * inv_rms * gain[i:i + 1, :]).astype(jnp.bfloat16))


def rope_tables(positions, head_dim):
    half_dim = head_dim // 2
    inv_freq = 10000.0 ** (-2.0 * jnp.arange(half_dim, dtype=jnp.float32) / head_dim)
    angles = positions.astype(jnp.float32)[:, None] * inv_freq[None, :]
    return jnp.cos(angles), jnp.sin(angles)


def plan_rows(cache_len):
    rows = cache_len.shape[0] // PARTS
    key = cache_len.reshape(PARTS, rows) * rows + jnp.arange(rows, dtype=jnp.int32)
    place = jnp.arange(rows + RING * GROUP, dtype=jnp.int32)
    rank = jnp.sum((key[:, None, :] < key[:, :, None]).astype(jnp.int32), axis=2)
    here = rank[:, None, :] == place[:, None]
    return jnp.sum(jnp.where(here, key[:, None, :], 0), axis=2)


def attend_kernel(part, plan_ref, x_ref, gm_ref, wo_hbm, k_hbm, v_hbm, *refs):
    if part == 0:
        (ga_ref, cos_ref, sin_ref, wq_hbm, wk_hbm, wv_hbm,
         xmid_ref, xn_ref, knew_ref, vnew_ref, qrest_ref,
         a_buf, wo_buf, o_buf, k_buf, v_buf, s_buf, kn_buf, vn_buf, wo_sem, k_sem, v_sem,
         in_buf, q_buf, wq_buf, wk_buf, wv_buf, wq_sem, wkv_sem) = refs
    else:
        (q_buf, knew_ref, vnew_ref, xmid_ref, xn_ref,
         a_buf, wo_buf, o_buf, k_buf, v_buf, s_buf, kn_buf, vn_buf, wo_sem, k_sem, v_sem) = refs
    rows, width = xmid_ref.shape
    cap, dim = k_hbm.shape[1:]
    heads = q_buf.shape[1] // rows
    row_base = part * rows
    num_groups = rows // GROUP
    num_blocks = width // PROJ_BLOCK
    per_block = PROJ_BLOCK // dim
    low, high = slice(0, dim // 2), slice(dim // 2, dim)

    def block_copy(src_hbm, dst_buf, sems, block):
        cols = pl.ds(pl.multiple_of(block * PROJ_BLOCK, PROJ_BLOCK), PROJ_BLOCK)
        return pltpu.make_async_copy(src_hbm.at[:, cols], dst_buf.at[block], sems.at[block])

    def length(place):
        return lax.div(plan_ref[part, place], rows)

    def row_of(place):
        return lax.rem(plan_ref[part, place], rows)

    def used(place):
        return pl.multiple_of((length(place) + (GRAIN - 1)) & ~(GRAIN - 1), GRAIN)

    def start(src_hbm, dst_buf, sems, group):
        ring = lax.rem(group, RING)
        for lane in range(GROUP):
            place = group * GROUP + lane
            base = pl.multiple_of((ring * GROUP + lane) * cap, cap)
            pltpu.make_async_copy(src_hbm.at[row_of(place) + row_base, pl.ds(0, used(place)), :],
                                  dst_buf.at[pl.ds(base, used(place)), :], sems.at[ring]).start()

    def wait(dst_buf, sems, group):
        ring = lax.rem(group, RING)
        total = sum(used(group * GROUP + lane) for lane in range(GROUP))
        whole = dst_buf.at[pl.ds(0, pl.multiple_of(total, GRAIN)), :]
        pltpu.make_async_copy(whole, whole, sems.at[ring]).wait()

    def head_rows(row):
        return pl.ds(pl.multiple_of(row * heads, heads), heads)

    def load_query(row):
        return jnp.concatenate([q_buf[0, head_rows(row), :], q_buf[1, head_rows(row), :]], axis=-1)

    def scores(group, span):
        ring = lax.rem(group, RING)
        for lane in range(GROUP):
            base = pl.multiple_of((ring * GROUP + lane) * cap, cap)
            query = load_query(row_of(group * GROUP + lane)).astype(jnp.bfloat16)
            s_buf[lax.rem(group, 2), lane, :, pl.ds(0, span)] = lax.dot_general(
                query, k_buf[pl.ds(base, span), :], (((1,), (1,)), ((), ())), preferred_element_type=jnp.float32)

    def outputs(group, span):
        ring = lax.rem(group, RING)
        column = lax.broadcasted_iota(jnp.int32, (heads, span), 1)
        for lane in range(GROUP):
            place = group * GROUP + lane
            row = row_of(place)
            base = pl.multiple_of((ring * GROUP + lane) * cap, cap)
            score = jnp.where(column < length(place), s_buf[lax.rem(group, 2), lane, :, pl.ds(0, span)], -jnp.inf)
            new_score = jnp.sum(load_query(row) * kn_buf[pl.ds(row, 1), :], axis=-1, keepdims=True)
            peak = jnp.maximum(jnp.max(score, axis=-1, keepdims=True), new_score)
            weight = jnp.exp(score - peak)
            new_weight = jnp.exp(new_score - peak)
            scale = 1.0 / (jnp.sum(weight, axis=-1, keepdims=True) + new_weight)
            prob = (weight * scale).astype(jnp.bfloat16)
            new_prob = (new_weight * scale).astype(jnp.bfloat16).astype(jnp.float32)
            mixed = jnp.dot(prob, v_buf[pl.ds(base, span), :], preferred_element_type=jnp.float32)
            mixed = mixed + new_prob * vn_buf[pl.ds(row, 1), :]
            o_buf[0, head_rows(row), :] = mixed[:, low]
            o_buf[1, head_rows(row), :] = mixed[:, high]

    def by_span(group, run):
        tiles = lax.div(length(group * GROUP + GROUP - 1) + (TILE - 1), TILE)
        for count in range(1, cap // TILE + 1):
            least = 0 if count == 1 else count

            @pl.when((tiles >= least) & (tiles <= count))
            def _(count=count):
                run(count * TILE)

    if part == 0:
        kv_copies = (pltpu.make_async_copy(wk_hbm, wk_buf, wkv_sem.at[0]),
                     pltpu.make_async_copy(wv_hbm, wv_buf, wkv_sem.at[1]))
        for copy in kv_copies:
            copy.start()
        for block in range(num_blocks):
            block_copy(wq_hbm, wq_buf, wq_sem, block).start()
    for group in range(RING):
        start(k_hbm, k_buf, k_sem, group)

    def clear(part, carry):
        span = pl.ds(pl.multiple_of(part * cap, cap), cap)
        v_buf[span, :] = jnp.zeros((cap, dim), v_buf.dtype)
        return carry

    lax.fori_loop(0, RING * GROUP, clear, 0)
    for group in range(RING):
        start(v_hbm, v_buf, v_sem, group)
    for block in range(num_blocks):
        block_copy(wo_hbm, wo_buf, wo_sem, block).start()

    def norm(from_ref, gain_ref, to_ref, count):
        def body(step, carry):
            span = pl.ds(pl.multiple_of(step * NORM_ROWS, NORM_ROWS), NORM_ROWS)

            def store(cols, values):
                to_ref[span, cols] = values

            rms_scale(from_ref[span, :], gain_ref, store)
            return carry

        lax.fori_loop(0, count // NORM_ROWS, body, 0)

    def turn(values):
        cos_t, sin_t = cos_ref[...], sin_ref[...]
        return (values[:, low] * cos_t - values[:, high] * sin_t,
                values[:, high] * cos_t + values[:, low] * sin_t)

    def project(block, carry):
        block_copy(wq_hbm, wq_buf, wq_sem, block).wait()
        lin = jnp.dot(in_buf[...], wq_buf[block], preferred_element_type=jnp.float32)
        for i in range(per_block):
            place = pl.ds(block * per_block + i, rows, stride=heads)
            for side, piece in enumerate(turn(lin[:, i * dim:(i + 1) * dim])):
                piece = (piece * dim ** -0.5).astype(jnp.bfloat16).astype(jnp.float32)
                q_buf[side, place, :] = piece[:rows]
                qrest_ref[side, place, :] = piece[rows:]
        return carry

    if part == 0:
        norm(x_ref, ga_ref, in_buf, PARTS * rows)
        for copy in kv_copies:
            copy.wait()
        k_lin = jnp.dot(in_buf[...], wk_buf[...], preferred_element_type=jnp.float32)
        for piece, span in zip(turn(k_lin), (low, high)):
            knew_ref[:, span] = piece.astype(jnp.bfloat16)
        vnew_ref[...] = jnp.dot(in_buf[...], wv_buf[...], preferred_element_type=jnp.float32).astype(jnp.bfloat16)
        lax.fori_loop(0, num_blocks, project, 0)
    kn_buf[...] = knew_ref[pl.ds(row_base, rows), :].astype(jnp.float32)
    vn_buf[...] = vnew_ref[pl.ds(row_base, rows), :].astype(jnp.float32)

    wait(k_buf, k_sem, 0)
    by_span(0, lambda span: scores(0, span))

    def step(group, carry):
        start(k_hbm, k_buf, k_sem, group + RING)
        wait(k_buf, k_sem, group + 1)
        wait(v_buf, v_sem, group)

        def run(span):
            scores(group + 1, span)
            outputs(group, span)

        by_span(group + 1, run)
        start(v_hbm, v_buf, v_sem, group + RING)
        return carry

    lax.fori_loop(0, num_groups - 1, step, 0)
    wait(v_buf, v_sem, num_groups - 1)
    by_span(num_groups - 1, lambda span: outputs(num_groups - 1, span))

    for head in range(heads):
        for side in range(2):
            first = head * dim + side * (dim // 2)
            a_buf[:, first:first + dim // 2] = o_buf[side, pl.ds(head, rows, stride=heads), :].astype(jnp.bfloat16)

    def mix(block, carry):
        block_copy(wo_hbm, wo_buf, wo_sem, block).wait()
        cols = pl.ds(pl.multiple_of(block * PROJ_BLOCK, PROJ_BLOCK), PROJ_BLOCK)
        mixed = jnp.dot(a_buf[...], wo_buf[block], preferred_element_type=jnp.float32)
        xmid_ref[:, cols] = x_ref[pl.ds(row_base, rows), cols].astype(jnp.float32) + mixed
        return carry

    lax.fori_loop(0, num_blocks, mix, 0)

    norm(xmid_ref, gm_ref, xn_ref, rows)


def attention_part(part, plan, hidden_in, k_cache, v_cache, norm_mlp, w_o, q_new=(), proj=()):
    cap, dim = k_cache.shape[1:]
    width = hidden_in.shape[1]
    rows = hidden_in.shape[0] // PARTS
    heads = w_o.shape[0] // dim
    num_blocks = width // PROJ_BLOCK
    smem = pl.BlockSpec(memory_space=pltpu.SMEM)
    vmem = pl.BlockSpec(memory_space=pltpu.VMEM)
    hbm = pl.BlockSpec(memory_space=pl.ANY)
    weights = [pltpu.VMEM((num_blocks, width, PROJ_BLOCK), jnp.bfloat16), pltpu.SemaphoreType.DMA((num_blocks,))]
    queries = (2, rows * heads, dim // 2)
    out_shape = [jax.ShapeDtypeStruct((rows, width), jnp.float32), jax.ShapeDtypeStruct((rows, width), jnp.bfloat16)]
    scratch_shapes = [
        pltpu.VMEM((rows, width), jnp.bfloat16),
        weights[0],
        pltpu.VMEM(queries, jnp.float32),
        pltpu.VMEM((RING * GROUP * cap, dim), jnp.bfloat16),
        pltpu.VMEM((RING * GROUP * cap, dim), jnp.bfloat16),
        pltpu.VMEM((2, GROUP, heads, cap), jnp.float32),
        pltpu.VMEM((rows, dim), jnp.float32),
        pltpu.VMEM((rows, dim), jnp.float32),
        weights[1],
        pltpu.SemaphoreType.DMA((RING,)),
        pltpu.SemaphoreType.DMA((RING,)),
    ]
    if part == 0:
        extra_specs = [vmem] * 3 + [hbm] * 3
        out_shape += [jax.ShapeDtypeStruct((PARTS * rows, dim), jnp.bfloat16)] * 2
        out_shape += [jax.ShapeDtypeStruct(queries, jnp.float32)]
        scratch_shapes += [
            pltpu.VMEM((PARTS * rows, width), jnp.bfloat16),
            pltpu.VMEM(queries, jnp.float32),
            weights[0],
            pltpu.VMEM((width, dim), jnp.bfloat16),
            pltpu.VMEM((width, dim), jnp.bfloat16),
            weights[1],
            pltpu.SemaphoreType.DMA((2,)),
        ]
    else:
        extra_specs = [vmem] * 3
    return pl.pallas_call(
        functools.partial(attend_kernel, part),
        name='attend',
        out_shape=out_shape,
        in_specs=[smem, vmem, vmem, hbm, hbm, hbm] + extra_specs,
        out_specs=[vmem] * len(out_shape),
        scratch_shapes=scratch_shapes,
        compiler_params=pltpu.CompilerParams(vmem_limit_bytes=62 * 1024 * 1024),
        cost_estimate=pl.CostEstimate(flops=4 * rows * width * width + 4 * rows * heads * dim * cap,
                                      bytes_accessed=2 * rows * cap * dim * 2 + 4 * width * width,
                                      transcendentals=rows * heads * cap),
    )(plan, hidden_in, norm_mlp.reshape(-1, LANES), w_o, k_cache, v_cache, *q_new, *proj)


HID_BLOCK = 512
OUT_BLOCK = 512
PAIR = 2
WEIGHT_RING = 2 * PAIR
MESH = pl.DeviceIdType.MESH
FAR, PARTNER, OWN = 0, 2, 3


def mlp_kernel(xn0_ref, xn1_ref, xmid0_ref, xmid1_ref, far_ref, wg_hbm, wu_hbm, wd_hbm, out_ref,
               x_all, h_buf, g_buf, u_buf, wg_buf, wu_buf, wd_buf, part, d_recv, c_recv, p_recv,
               w_sem, wd_sem, send_sem, recv_sem):
    half, width = xn0_ref.shape
    rows = 2 * half
    hidden = wg_hbm.shape[1]
    num_hid = hidden // HID_BLOCK
    num_pairs = num_hid // PAIR
    num_out = width // OUT_BLOCK
    num_steps = 4 * num_hid
    me = lax.axis_index('tp')
    partner = me + 1 - 2 * lax.rem(me, 2)
    counter = lax.rem(me + 2, 4)

    barrier = pltpu.get_barrier_semaphore()
    for peer in (partner, counter):
        pl.semaphore_signal(barrier, inc=1, device_id={'tp': peer}, device_id_type=MESH)

    def weight_copies(step):
        slot = lax.rem(step, WEIGHT_RING)
        cols = pl.ds(pl.multiple_of(lax.rem(step, num_hid) * HID_BLOCK, HID_BLOCK), HID_BLOCK)
        return (pltpu.make_async_copy(wg_hbm.at[:, cols], wg_buf.at[slot], w_sem.at[slot, 0]),
                pltpu.make_async_copy(wu_hbm.at[:, cols], wu_buf.at[slot], w_sem.at[slot, 1]))

    def down_copy(block):
        cols = pl.ds(pl.multiple_of(block * OUT_BLOCK, OUT_BLOCK), OUT_BLOCK)
        return pltpu.make_async_copy(wd_hbm.at[:, cols], wd_buf.at[block], wd_sem.at[block])

    def remote(src, dst, index, peer):
        return pltpu.make_async_remote_copy(
            src_ref=src, dst_ref=dst, send_sem=send_sem.at[index], recv_sem=recv_sem.at[index],
            device_id={'tp': peer}, device_id_type=MESH)

    top, bottom = pl.ds(0, half), pl.ds(half, half)
    gather_partner = [remote(ref, x_all.at[PARTNER, span, :], i, partner)
                      for i, (ref, span) in enumerate(((xn0_ref, top), (xn1_ref, bottom)))]
    gather_counter = remote(xn1_ref, x_all.at[FAR + 1, top, :], 2, counter)
    forward = [remote(far_ref, x_all.at[FAR, bottom, :], 3, partner),
               remote(x_all.at[FAR + 1, top, :], x_all.at[FAR + 1, bottom, :], 4, partner)]

    def cross(i, n):
        return remote(part.at[FAR + i, n, bottom, :], d_recv.at[i, n], 5 + i * num_out + n, partner)

    def home(i, n):
        return remote(part.at[FAR + i, n, top, :], c_recv.at[i, n], 5 + (2 + i) * num_out + n, counter)

    def side(n):
        return remote(part.at[PARTNER, n], p_recv.at[n], 5 + 4 * num_out + n, partner)

    for step in range(WEIGHT_RING):
        for copy in weight_copies(step):
            copy.start()
    pl.semaphore_wait(barrier, 2)
    forward[0].start()
    gather_counter.start()
    for copy in gather_partner:
        copy.start()
    x_all[FAR, top, :] = far_ref[...]
    x_all[OWN, top, :] = xn0_ref[...]
    x_all[OWN, bottom, :] = xn1_ref[...]

    def activate(keep, pair):
        for b in range(PAIR):
            first = (pair * PAIR + b) * HID_BLOCK
            cols = pl.ds(first if isinstance(first, int) else pl.multiple_of(first, HID_BLOCK), HID_BLOCK)
            h_buf[:, cols] = (jax.nn.gelu(g_buf[keep, b], approximate=True) * u_buf[keep, b]).astype(jnp.bfloat16)

    def down(number, n):
        part[number, n] = jnp.dot(h_buf[:, :hidden], wd_buf[n], preferred_element_type=jnp.float32)

    def finish(i, n):
        cross(i, n).wait_recv()
        part[FAR + i, n, top, :] = part[FAR + i, n, top, :] + d_recv[i, n]
        home(i, n).start()

    def one_pass(number, carry):
        is_partner = number == PARTNER
        is_far = number < PARTNER
        far = number - FAR

        @pl.when(is_partner)
        def _():
            for copy in gather_partner:
                copy.wait_recv()

        for i in range(2):
            @pl.when(number == FAR + i)
            def _(i=i):
                forward[i].wait_recv()

        def hidden_pair(pair, carry):
            first = number * num_hid + pair * PAIR
            keep = lax.rem(pair, 2)

            @pl.when(number == 0)
            def _():
                down_copy(pair).start()

            for b in range(PAIR):
                for copy in weight_copies(first + b):
                    copy.wait()
            for b in range(PAIR):
                slot = lax.rem(first + b, WEIGHT_RING)
                g_buf[keep, b] = jnp.dot(x_all[number], wg_buf[slot], preferred_element_type=jnp.float32)
                u_buf[keep, b] = jnp.dot(x_all[number], wu_buf[slot], preferred_element_type=jnp.float32)
                for copy in weight_copies(first + b + WEIGHT_RING):
                    copy.start()
            activate(1 - keep, lax.rem(pair + num_pairs, num_pairs + 1))

            @pl.when((pair == 0) & (number > FAR) & (number <= PARTNER))
            def _():
                for n in range(num_out // 2, num_out):
                    finish(far - 1, n)
            return carry

        lax.fori_loop(0, num_pairs, hidden_pair, 0)

        @pl.when(number == 0)
        def _():
            for n in range(num_out):
                down_copy(n).wait()

        activate((num_pairs - 1) % 2, num_pairs - 1)
        for n in range(num_out // 2):
            down(number, n)

        @pl.when(is_partner)
        def _():
            for n in range(num_out // 2):
                side(n).start()

        @pl.when(is_far)
        def _():
            for n in range(num_out // 2):
                cross(far, n).start()

        for n in range(num_out // 2, num_out):
            down(number, n)

        @pl.when(is_partner)
        def _():
            for n in range(num_out // 2, num_out):
                side(n).start()

        @pl.when(is_far)
        def _():
            for n in range(num_out // 2, num_out):
                cross(far, n).start()
            for n in range(num_out // 2):
                finish(far, n)

        @pl.when(number == FAR)
        def _():
            gather_counter.wait_recv()
            forward[1].start()
        return carry

    lax.fori_loop(0, 4, one_pass, 0)

    xmid = (xmid0_ref, xmid1_ref)

    def settle(n, carry):
        cols = pl.ds(pl.multiple_of(n * OUT_BLOCK, OUT_BLOCK), OUT_BLOCK)
        side(n).wait_recv()
        for i in range(2):
            span = pl.ds(i * half, half)
            home(i, n).wait_recv()
            total = part[OWN, n, span, :] + p_recv[n, span, :] + c_recv[i, n]
            out_ref[span, cols] = (xmid[i][:, cols] + total).astype(jnp.bfloat16)
        return carry

    lax.fori_loop(0, num_out, settle, 0)

    for step in range(num_steps, num_steps + WEIGHT_RING):
        for copy in weight_copies(step):
            copy.wait()
    gather_counter.wait_send()
    for i in range(2):
        gather_partner[i].wait_send()
        forward[i].wait_send()

    def drain(n, carry):
        side(n).wait_send()
        for i in range(2):
            cross(i, n).wait_send()
            home(i, n).wait_send()
        return carry

    lax.fori_loop(0, num_out, drain, 0)


def mlp_block(xn_mid, x_mid, far, w_gate, w_up, w_down):
    half, width = far.shape
    rows = 2 * half
    hidden = w_gate.shape[1]
    num_out = width // OUT_BLOCK
    num_copies = 5 + 5 * num_out
    vmem = pl.BlockSpec(memory_space=pltpu.VMEM)
    hbm = pl.BlockSpec(memory_space=pl.ANY)
    return pl.pallas_call(
        mlp_kernel,
        name='mlp',
        out_shape=jax.ShapeDtypeStruct((rows, width), jnp.bfloat16),
        in_specs=[vmem] * 5 + [hbm] * 3,
        out_specs=vmem,
        scratch_shapes=[
            pltpu.VMEM((4, rows, width), jnp.bfloat16),
            pltpu.VMEM((rows, hidden + PAIR * HID_BLOCK), jnp.bfloat16),
            pltpu.VMEM((2, PAIR, rows, HID_BLOCK), jnp.float32),
            pltpu.VMEM((2, PAIR, rows, HID_BLOCK), jnp.float32),
            pltpu.VMEM((WEIGHT_RING, width, HID_BLOCK), jnp.bfloat16),
            pltpu.VMEM((WEIGHT_RING, width, HID_BLOCK), jnp.bfloat16),
            pltpu.VMEM((num_out, hidden, OUT_BLOCK), jnp.bfloat16),
            pltpu.VMEM((4, num_out, rows, OUT_BLOCK), jnp.float32),
            pltpu.VMEM((2, num_out, half, OUT_BLOCK), jnp.float32),
            pltpu.VMEM((2, num_out, half, OUT_BLOCK), jnp.float32),
            pltpu.VMEM((num_out, rows, OUT_BLOCK), jnp.float32),
            pltpu.SemaphoreType.DMA((WEIGHT_RING, 2)),
            pltpu.SemaphoreType.DMA((num_out,)),
            pltpu.SemaphoreType.DMA((num_copies,)),
            pltpu.SemaphoreType.DMA((num_copies,)),
        ],
        compiler_params=pltpu.CompilerParams(collective_id=0, has_side_effects=True,
                                             vmem_limit_bytes=67043328),
        cost_estimate=pl.CostEstimate(flops=24 * rows * width * hidden,
                                      bytes_accessed=9 * width * hidden * 2,
                                      transcendentals=4 * rows * hidden),
    )(*xn_mid, *x_mid, far, w_gate, w_up, w_down)


def solution(mesh):
    row_spec = P(('dp', 'tp'), None)
    cache_spec = P(('dp', 'tp'), None, None)
    full_vec = P(None)
    full_mat = P(None, None)

    def per_device(hidden_in, k_cache, v_cache, cache_len, norm_attn, norm_mlp, w_q, w_k, w_v, w_o, w_gate, w_up, w_down):
        cos_t, sin_t = rope_tables(cache_len, w_k.shape[1])
        plan = plan_rows(cache_len)
        common = (plan, hidden_in, k_cache, v_cache, norm_mlp, w_o)
        x_first, xn_first, k_new, v_new, q_rest = attention_part(
            0, *common, proj=(norm_attn.reshape(-1, LANES), cos_t, sin_t, w_q, w_k, w_v))
        far = lax.ppermute(xn_first, 'tp', [(0, 2), (1, 3), (2, 0), (3, 1)])
        x_last, xn_last = attention_part(1, *common, q_new=(q_rest, k_new, v_new))
        hidden_out = mlp_block((xn_first, xn_last), (x_first, x_last), far, w_gate, w_up, w_down)
        return hidden_out, k_new, v_new

    return jax.shard_map(
        per_device,
        mesh=mesh,
        in_specs=(row_spec, cache_spec, cache_spec, P(('dp', 'tp')), full_vec, full_vec,
                  full_mat, full_mat, full_mat, full_mat, P(None, 'tp'), P(None, 'tp'), P('tp', None)),
        out_specs=(row_spec, row_spec, row_spec),
        check_vma=False,
    )
```

```python
import functools

import jax
import jax.numpy as jnp
from jax import lax
from jax.experimental import pallas as pl
from jax.experimental.pallas import tpu as pltpu
from jax.sharding import PartitionSpec as P

GROUP = 16
RING = 4
GRAIN = 16
TILE = 128
PROJ_BLOCK = 512
NORM_ROWS = 32
LANES = 128
PARTS = 2


def rms_scale(values, gain_ref, store):
    wide_vals = values.astype(jnp.float32)
    inv_rms = lax.rsqrt(jnp.mean(wide_vals * wide_vals, axis=-1, keepdims=True) + 1e-6)
    gain = 1.0 + gain_ref[...].astype(jnp.float32)
    for i in range(gain.shape[0]):
        cols = slice(i * LANES, (i + 1) * LANES)
        store(cols, (wide_vals[:, cols] * inv_rms * gain[i:i + 1, :]).astype(jnp.bfloat16))


def rope_tables(positions, head_dim):
    half_dim = head_dim // 2
    inv_freq = 10000.0 ** (-2.0 * jnp.arange(half_dim, dtype=jnp.float32) / head_dim)
    angles = positions.astype(jnp.float32)[:, None] * inv_freq[None, :]
    return jnp.cos(angles), jnp.sin(angles)


def plan_rows(cache_len):
    rows = cache_len.shape[0] // PARTS
    key = cache_len.reshape(PARTS, rows) * rows + jnp.arange(rows, dtype=jnp.int32)
    place = jnp.arange(rows + RING * GROUP, dtype=jnp.int32)
    rank = jnp.sum((key[:, None, :] > key[:, :, None]).astype(jnp.int32), axis=2)
    here = rank[:, None, :] == place[:, None]
    return jnp.sum(jnp.where(here, key[:, None, :], 0), axis=2)


def attend_kernel(part, plan_ref, x_ref, gm_ref, wo_hbm, k_hbm, v_hbm, *refs):
    if part == 0:
        (ga_ref, cos_ref, sin_ref, wq_hbm, wk_hbm, wv_hbm,
         xmid_ref, xn_ref, knew_ref, vnew_ref, qrest_ref,
         a_buf, wo_buf, o_buf, k_buf, v_buf, s_buf, kn_buf, vn_buf, wo_sem, k_sem, v_sem,
         in_buf, q_buf, wq_buf, wk_buf, wv_buf, wq_sem, wkv_sem) = refs
    else:
        (q_hbm, knew_hbm, vnew_hbm, xmid_ref, xn_ref,
         a_buf, wo_buf, o_buf, k_buf, v_buf, s_buf, kn_buf, vn_buf, wo_sem, k_sem, v_sem,
         x_buf, q_buf, knew_buf, vnew_buf, in_sem) = refs
    rows, width = xmid_ref.shape
    cap, dim = k_hbm.shape[1:]
    heads = q_buf.shape[1] // rows
    row_base = part * rows
    num_groups = rows // GROUP
    num_blocks = width // PROJ_BLOCK
    per_block = PROJ_BLOCK // dim
    low, high = slice(0, dim // 2), slice(dim // 2, dim)

    def block_copy(src_hbm, dst_buf, sems, block):
        cols = pl.ds(pl.multiple_of(block * PROJ_BLOCK, PROJ_BLOCK), PROJ_BLOCK)
        return pltpu.make_async_copy(src_hbm.at[:, cols], dst_buf.at[block], sems.at[block])

    assert rows & (rows - 1) == 0 and TILE & (TILE - 1) == 0 and RING & (RING - 1) == 0
    row_bits, tile_bits = rows.bit_length() - 1, TILE.bit_length() - 1

    def length(place):
        return plan_ref[part, place] >> row_bits

    def row_of(place):
        return plan_ref[part, place] & (rows - 1)

    def used(place):
        return pl.multiple_of((length(place) + (GRAIN - 1)) & ~(GRAIN - 1), GRAIN)

    def tiles_of(group):
        return jnp.maximum((length(group * GROUP) + (TILE - 1)) >> tile_bits, 1)

    def start(src_hbm, dst_buf, sems, group):
        ring = group & (RING - 1)
        for lane in range(GROUP):
            place = group * GROUP + lane
            base = pl.multiple_of((ring * GROUP + lane) * cap, cap)
            pltpu.make_async_copy(src_hbm.at[row_of(place) + row_base, pl.ds(0, used(place)), :],
                                  dst_buf.at[pl.ds(base, used(place)), :], sems.at[ring]).start()

    def wait(dst_buf, sems, group):
        ring = group & (RING - 1)
        total = sum(used(group * GROUP + lane) for lane in range(GROUP))
        whole = dst_buf.at[pl.ds(0, pl.multiple_of(total, GRAIN)), :]
        pltpu.make_async_copy(whole, whole, sems.at[ring]).wait()

    def head_rows(row):
        return pl.ds(pl.multiple_of(row * heads, heads), heads)

    def load_query(row):
        return jnp.concatenate([q_buf[0, head_rows(row), :], q_buf[1, head_rows(row), :]], axis=-1)

    def scores(group, span):
        ring = group & (RING - 1)
        for lane in range(GROUP):
            base = pl.multiple_of((ring * GROUP + lane) * cap, cap)
            query = load_query(row_of(group * GROUP + lane)).astype(jnp.bfloat16)
            s_buf[group & 1, lane, :, pl.ds(0, span)] = lax.dot_general(
                query, k_buf[pl.ds(base, span), :], (((1,), (1,)), ((), ())), preferred_element_type=jnp.float32)

    def outputs(group, span):
        ring = group & (RING - 1)
        column = lax.broadcasted_iota(jnp.int32, (heads, span), 1)
        for lane in range(GROUP):
            place = group * GROUP + lane
            row = row_of(place)
            base = pl.multiple_of((ring * GROUP + lane) * cap, cap)
            score = jnp.where(column < length(place), s_buf[group & 1, lane, :, pl.ds(0, span)], -jnp.inf)
            new_score = jnp.sum(load_query(row) * kn_buf[pl.ds(row, 1), :], axis=-1, keepdims=True)
            peak = jnp.maximum(jnp.max(score, axis=-1, keepdims=True), new_score)
            weight = jnp.exp(score - peak)
            new_weight = jnp.exp(new_score - peak)
            scale = 1.0 / (jnp.sum(weight, axis=-1, keepdims=True) + new_weight)
            prob = (weight * scale).astype(jnp.bfloat16)
            new_prob = (new_weight * scale).astype(jnp.bfloat16).astype(jnp.float32)
            mixed = jnp.dot(prob, v_buf[pl.ds(base, span), :], preferred_element_type=jnp.float32)
            mixed = mixed + new_prob * vn_buf[pl.ds(row, 1), :]
            o_buf[0, head_rows(row), :] = mixed[:, low]
            o_buf[1, head_rows(row), :] = mixed[:, high]

    def by_span(group, run):
        tiles = tiles_of(group)
        for count in range(1, cap // TILE + 1):
            @pl.when(tiles == count)
            def _(count=count):
                run(count * TILE)

    if part == 0:
        kv_copies = (pltpu.make_async_copy(wk_hbm, wk_buf, wkv_sem.at[0]),
                     pltpu.make_async_copy(wv_hbm, wv_buf, wkv_sem.at[1]))
        for copy in kv_copies:
            copy.start()
        for block in range(num_blocks):
            block_copy(wq_hbm, wq_buf, wq_sem, block).start()
    else:
        own = pl.ds(row_base, rows)
        in_copies = [pltpu.make_async_copy(src, dst, in_sem.at[i]) for i, (src, dst) in enumerate((
            (q_hbm, q_buf), (knew_hbm.at[own, :], knew_buf), (vnew_hbm.at[own, :], vnew_buf),
            (x_ref.at[own, :], x_buf)))]
        for copy in in_copies:
            copy.start()
    def clear(place, carry):
        def body(tile, carry):
            span = pl.ds(pl.multiple_of(place * cap + tile * TILE, TILE), TILE)
            v_buf[span, :] = jnp.zeros((TILE, dim), v_buf.dtype)
            return carry

        return lax.fori_loop(used(place) >> tile_bits, tiles_of(place // GROUP), body, carry)

    def fill(group, carry):
        start(k_hbm, k_buf, k_sem, group)
        lax.fori_loop(group * GROUP, (group + 1) * GROUP, clear, 0)
        start(v_hbm, v_buf, v_sem, group)
        return carry

    lax.fori_loop(0, RING, fill, 0)
    for block in range(num_blocks):
        block_copy(wo_hbm, wo_buf, wo_sem, block).start()

    def norm(from_ref, gain_ref, to_ref, count):
        def body(step, carry):
            span = pl.ds(pl.multiple_of(step * NORM_ROWS, NORM_ROWS), NORM_ROWS)

            def store(cols, values):
                to_ref[span, cols] = values

            rms_scale(from_ref[span, :], gain_ref, store)
            return carry

        lax.fori_loop(0, count // NORM_ROWS, body, 0)

    def turn(values):
        cos_t, sin_t = cos_ref[...], sin_ref[...]
        return (values[:, low] * cos_t - values[:, high] * sin_t,
                values[:, high] * cos_t + values[:, low] * sin_t)

    def project(block, carry):
        block_copy(wq_hbm, wq_buf, wq_sem, block).wait()
        lin = jnp.dot(in_buf[...], wq_buf[block], preferred_element_type=jnp.float32)
        for i in range(per_block):
            place = pl.ds(block * per_block + i, rows, stride=heads)
            for side, piece in enumerate(turn(lin[:, i * dim:(i + 1) * dim])):
                piece = (piece * dim ** -0.5).astype(jnp.bfloat16).astype(jnp.float32)
                q_buf[side, place, :] = piece[:rows]
                qrest_ref[side, place, :] = piece[rows:]
        return carry

    if part == 0:
        norm(x_ref, ga_ref, in_buf, PARTS * rows)
        for copy in kv_copies:
            copy.wait()
        k_lin = jnp.dot(in_buf[...], wk_buf[...], preferred_element_type=jnp.float32)
        for piece, span in zip(turn(k_lin), (low, high)):
            knew_ref[:, span] = piece.astype(jnp.bfloat16)
        vnew_ref[...] = jnp.dot(in_buf[...], wv_buf[...], preferred_element_type=jnp.float32).astype(jnp.bfloat16)
        lax.fori_loop(0, num_blocks, project, 0)
        kn_buf[...] = knew_ref[pl.ds(0, rows), :].astype(jnp.float32)
        vn_buf[...] = vnew_ref[pl.ds(0, rows), :].astype(jnp.float32)
        x_own = x_ref.at[pl.ds(0, rows), :]
    else:
        for copy in in_copies:
            copy.wait()
        kn_buf[...] = knew_buf[...].astype(jnp.float32)
        vn_buf[...] = vnew_buf[...].astype(jnp.float32)
        x_own = x_buf

    wait(k_buf, k_sem, 0)
    by_span(0, lambda span: scores(0, span))

    def step(group, carry):
        wait(k_buf, k_sem, group + 1)
        wait(v_buf, v_sem, group)

        def run(span):
            scores(group + 1, span)
            outputs(group, span)
            start(k_hbm, k_buf, k_sem, group + RING)
            start(v_hbm, v_buf, v_sem, group + RING)

        by_span(group, run)
        return carry

    lax.fori_loop(0, num_groups - 1, step, 0)
    wait(v_buf, v_sem, num_groups - 1)
    by_span(num_groups - 1, lambda span: outputs(num_groups - 1, span))

    for head in range(heads):
        for side in range(2):
            first = head * dim + side * (dim // 2)
            a_buf[:, first:first + dim // 2] = o_buf[side, pl.ds(head, rows, stride=heads), :].astype(jnp.bfloat16)

    def mix(block, carry):
        block_copy(wo_hbm, wo_buf, wo_sem, block).wait()
        cols = pl.ds(pl.multiple_of(block * PROJ_BLOCK, PROJ_BLOCK), PROJ_BLOCK)
        mixed = jnp.dot(a_buf[...], wo_buf[block], preferred_element_type=jnp.float32)
        xmid_ref[:, cols] = x_own[:, cols].astype(jnp.float32) + mixed
        return carry

    lax.fori_loop(0, num_blocks, mix, 0)

    norm(xmid_ref, gm_ref, xn_ref, rows)


def attention_part(part, plan, hidden_in, k_cache, v_cache, norm_mlp, w_o, q_new=(), proj=()):
    cap, dim = k_cache.shape[1:]
    width = hidden_in.shape[1]
    rows = hidden_in.shape[0] // PARTS
    heads = w_o.shape[0] // dim
    num_blocks = width // PROJ_BLOCK
    smem = pl.BlockSpec(memory_space=pltpu.SMEM)
    vmem = pl.BlockSpec(memory_space=pltpu.VMEM)
    hbm = pl.BlockSpec(memory_space=pl.ANY)
    weights = [pltpu.VMEM((num_blocks, width, PROJ_BLOCK), jnp.bfloat16), pltpu.SemaphoreType.DMA((num_blocks,))]
    queries = (2, rows * heads, dim // 2)
    out_shape = [jax.ShapeDtypeStruct((rows, width), jnp.float32), jax.ShapeDtypeStruct((rows, width), jnp.bfloat16)]
    scratch_shapes = [
        pltpu.VMEM((rows, width), jnp.bfloat16),
        weights[0],
        pltpu.VMEM(queries, jnp.float32),
        pltpu.VMEM((RING * GROUP * cap, dim), jnp.bfloat16),
        pltpu.VMEM((RING * GROUP * cap, dim), jnp.bfloat16),
        pltpu.VMEM((2, GROUP, heads, cap), jnp.float32),
        pltpu.VMEM((rows, dim), jnp.float32),
        pltpu.VMEM((rows, dim), jnp.float32),
        weights[1],
        pltpu.SemaphoreType.DMA((RING,)),
        pltpu.SemaphoreType.DMA((RING,)),
    ]
    if part == 0:
        extra_specs = [vmem] * 3 + [hbm] * 3
        out_shape += [jax.ShapeDtypeStruct((PARTS * rows, dim), jnp.bfloat16)] * 2
        out_shape += [jax.ShapeDtypeStruct(queries, jnp.float32)]
        scratch_shapes += [
            pltpu.VMEM((PARTS * rows, width), jnp.bfloat16),
            pltpu.VMEM(queries, jnp.float32),
            weights[0],
            pltpu.VMEM((width, dim), jnp.bfloat16),
            pltpu.VMEM((width, dim), jnp.bfloat16),
            weights[1],
            pltpu.SemaphoreType.DMA((2,)),
        ]
    else:
        extra_specs = [hbm] * 3
        scratch_shapes += [
            pltpu.VMEM((rows, width), jnp.bfloat16),
            pltpu.VMEM(queries, jnp.float32),
            pltpu.VMEM((rows, dim), jnp.bfloat16),
            pltpu.VMEM((rows, dim), jnp.bfloat16),
            pltpu.SemaphoreType.DMA((4,)),
        ]
    return pl.pallas_call(
        functools.partial(attend_kernel, part),
        name='attend',
        out_shape=out_shape,
        in_specs=[smem, hbm if part else vmem, vmem, hbm, hbm, hbm] + extra_specs,
        out_specs=[vmem] * len(out_shape),
        scratch_shapes=scratch_shapes,
        compiler_params=pltpu.CompilerParams(vmem_limit_bytes=67043328),
        cost_estimate=pl.CostEstimate(flops=4 * rows * width * width + 4 * rows * heads * dim * cap,
                                      bytes_accessed=2 * rows * cap * dim * 2 + 4 * width * width,
                                      transcendentals=rows * heads * cap),
    )(plan, hidden_in, norm_mlp.reshape(-1, LANES), w_o, k_cache, v_cache, *q_new, *proj)


HID_BLOCK = 512
OUT_BLOCK = 512
PAIR = 2
WEIGHT_RING = 2 * PAIR
MESH = pl.DeviceIdType.MESH
FAR, PARTNER, OWN = 0, 2, 3


def mlp_kernel(xn0_ref, xn1_ref, xmid0_ref, xmid1_ref, far_ref, wg_hbm, wu_hbm, wd_hbm, out_ref,
               x_all, h_buf, g_buf, u_buf, wg_buf, wu_buf, wd_buf, part, d_recv, c_recv, p_recv,
               xmid_buf, w_sem, wd_sem, in_sem, send_sem, recv_sem):
    half, width = xn0_ref.shape
    rows = 2 * half
    hidden = wg_hbm.shape[1]
    num_hid = hidden // HID_BLOCK
    num_pairs = num_hid // PAIR
    num_out = width // OUT_BLOCK
    num_steps = 4 * num_hid
    me = lax.axis_index('tp')
    partner = me + 1 - 2 * lax.rem(me, 2)
    counter = lax.rem(me + 2, 4)

    barrier = pltpu.get_barrier_semaphore()
    for peer in (partner, counter):
        pl.semaphore_signal(barrier, inc=1, device_id={'tp': peer}, device_id_type=MESH)

    def weight_copies(step):
        slot = lax.rem(step, WEIGHT_RING)
        cols = pl.ds(pl.multiple_of(lax.rem(step, num_hid) * HID_BLOCK, HID_BLOCK), HID_BLOCK)
        return (pltpu.make_async_copy(wg_hbm.at[:, cols], wg_buf.at[slot], w_sem.at[slot, 0]),
                pltpu.make_async_copy(wu_hbm.at[:, cols], wu_buf.at[slot], w_sem.at[slot, 1]))

    def down_copy(block):
        cols = pl.ds(pl.multiple_of(block * OUT_BLOCK, OUT_BLOCK), OUT_BLOCK)
        return pltpu.make_async_copy(wd_hbm.at[:, cols], wd_buf.at[block], wd_sem.at[block])

    def remote(src, dst, index, peer):
        return pltpu.make_async_remote_copy(
            src_ref=src, dst_ref=dst, send_sem=send_sem.at[index], recv_sem=recv_sem.at[index],
            device_id={'tp': peer}, device_id_type=MESH)

    top, bottom = pl.ds(0, half), pl.ds(half, half)
    gather_partner = [remote(ref, x_all.at[PARTNER, span, :], i, partner)
                      for i, (ref, span) in enumerate(((xn0_ref, top), (xn1_ref, bottom)))]
    gather_counter = remote(xn1_ref, x_all.at[FAR + 1, top, :], 2, counter)
    forward = [remote(far_ref, x_all.at[FAR, bottom, :], 3, partner),
               remote(x_all.at[FAR + 1, top, :], x_all.at[FAR + 1, bottom, :], 4, partner)]

    def cross(i, n):
        return remote(part.at[FAR + i, n, bottom, :], d_recv.at[i, n], 5 + i * num_out + n, partner)

    def home(i, n):
        return remote(part.at[FAR + i, n, top, :], c_recv.at[i, n], 5 + (2 + i) * num_out + n, counter)

    def side(n):
        return remote(part.at[PARTNER, n], p_recv.at[n], 5 + 4 * num_out + n, partner)

    for step in range(WEIGHT_RING):
        for copy in weight_copies(step):
            copy.start()
    in_copies = [pltpu.make_async_copy(ref, dst, in_sem.at[i]) for i, (ref, dst) in enumerate((
        (far_ref, x_all.at[FAR, top, :]), (xn0_ref, x_all.at[OWN, top, :]), (xn1_ref, x_all.at[OWN, bottom, :]),
        (xmid0_ref, xmid_buf.at[0]), (xmid1_ref, xmid_buf.at[1])))]
    for copy in in_copies:
        copy.start()
    pl.semaphore_wait(barrier, 2)
    forward[0].start()
    gather_counter.start()
    for copy in gather_partner:
        copy.start()

    def activate(keep, pair):
        for b in range(PAIR):
            first = (pair * PAIR + b) * HID_BLOCK
            cols = pl.ds(first if isinstance(first, int) else pl.multiple_of(first, HID_BLOCK), HID_BLOCK)
            h_buf[:, cols] = (jax.nn.gelu(g_buf[keep, b], approximate=True) * u_buf[keep, b]).astype(jnp.bfloat16)

    def down(number, n):
        part[number, n] = jnp.dot(h_buf[:, :hidden], wd_buf[n], preferred_element_type=jnp.float32)

    def finish(i, n):
        cross(i, n).wait_recv()
        part[FAR + i, n, top, :] = part[FAR + i, n, top, :] + d_recv[i, n]
        home(i, n).start()

    def one_pass(number, carry):
        is_partner = number == PARTNER
        is_far = number < PARTNER
        far = number - FAR

        @pl.when(number == 0)
        def _():
            in_copies[0].wait()

        @pl.when(is_partner)
        def _():
            for copy in gather_partner:
                copy.wait_recv()

        @pl.when(number == OWN)
        def _():
            for copy in in_copies[1:3]:
                copy.wait()

        for i in range(2):
            @pl.when(number == FAR + i)
            def _(i=i):
                forward[i].wait_recv()

        def hidden_pair(pair, carry):
            first = number * num_hid + pair * PAIR
            keep = lax.rem(pair, 2)

            @pl.when(number == 0)
            def _():
                down_copy(pair).start()

            for b in range(PAIR):
                for copy in weight_copies(first + b):
                    copy.wait()
            for b in range(PAIR):
                slot = lax.rem(first + b, WEIGHT_RING)
                g_buf[keep, b] = jnp.dot(x_all[number], wg_buf[slot], preferred_element_type=jnp.float32)
                u_buf[keep, b] = jnp.dot(x_all[number], wu_buf[slot], preferred_element_type=jnp.float32)
                for copy in weight_copies(first + b + WEIGHT_RING):
                    copy.start()
            activate(1 - keep, lax.rem(pair + num_pairs, num_pairs + 1))

            @pl.when((pair == 0) & (number > FAR) & (number <= PARTNER))
            def _():
                for n in range(num_out // 2, num_out):
                    finish(far - 1, n)
            return carry

        lax.fori_loop(0, num_pairs, hidden_pair, 0)

        @pl.when(number == 0)
        def _():
            for n in range(num_out):
                down_copy(n).wait()

        activate((num_pairs - 1) % 2, num_pairs - 1)
        for n in range(num_out // 2):
            down(number, n)

        @pl.when(is_partner)
        def _():
            for n in range(num_out // 2):
                side(n).start()

        @pl.when(is_far)
        def _():
            for n in range(num_out // 2):
                cross(far, n).start()

        for n in range(num_out // 2, num_out):
            down(number, n)

        @pl.when(is_partner)
        def _():
            for n in range(num_out // 2, num_out):
                side(n).start()

        @pl.when(is_far)
        def _():
            for n in range(num_out // 2, num_out):
                cross(far, n).start()
            for n in range(num_out // 2):
                finish(far, n)

        @pl.when(number == FAR)
        def _():
            gather_counter.wait_recv()
            forward[1].start()
        return carry

    lax.fori_loop(0, 4, one_pass, 0)

    for copy in in_copies[3:]:
        copy.wait()

    def settle(n, carry):
        cols = pl.ds(pl.multiple_of(n * OUT_BLOCK, OUT_BLOCK), OUT_BLOCK)
        side(n).wait_recv()
        for i in range(2):
            span = pl.ds(i * half, half)
            home(i, n).wait_recv()
            total = part[OWN, n, span, :] + p_recv[n, span, :] + c_recv[i, n]
            out_ref[span, cols] = (xmid_buf[i, :, cols] + total).astype(jnp.bfloat16)
        return carry

    lax.fori_loop(0, num_out, settle, 0)

    for step in range(num_steps, num_steps + WEIGHT_RING):
        for copy in weight_copies(step):
            copy.wait()
    gather_counter.wait_send()
    for i in range(2):
        gather_partner[i].wait_send()
        forward[i].wait_send()

    def drain(n, carry):
        side(n).wait_send()
        for i in range(2):
            cross(i, n).wait_send()
            home(i, n).wait_send()
        return carry

    lax.fori_loop(0, num_out, drain, 0)


def mlp_block(xn_mid, x_mid, far, w_gate, w_up, w_down):
    half, width = far.shape
    rows = 2 * half
    hidden = w_gate.shape[1]
    num_out = width // OUT_BLOCK
    num_copies = 5 + 5 * num_out
    vmem = pl.BlockSpec(memory_space=pltpu.VMEM)
    hbm = pl.BlockSpec(memory_space=pl.ANY)
    return pl.pallas_call(
        mlp_kernel,
        name='mlp',
        out_shape=jax.ShapeDtypeStruct((rows, width), jnp.bfloat16),
        in_specs=[hbm] * 8,
        out_specs=vmem,
        scratch_shapes=[
            pltpu.VMEM((4, rows, width), jnp.bfloat16),
            pltpu.VMEM((rows, hidden + PAIR * HID_BLOCK), jnp.bfloat16),
            pltpu.VMEM((2, PAIR, rows, HID_BLOCK), jnp.float32),
            pltpu.VMEM((2, PAIR, rows, HID_BLOCK), jnp.float32),
            pltpu.VMEM((WEIGHT_RING, width, HID_BLOCK), jnp.bfloat16),
            pltpu.VMEM((WEIGHT_RING, width, HID_BLOCK), jnp.bfloat16),
            pltpu.VMEM((num_out, hidden, OUT_BLOCK), jnp.bfloat16),
            pltpu.VMEM((4, num_out, rows, OUT_BLOCK), jnp.float32),
            pltpu.VMEM((2, num_out, half, OUT_BLOCK), jnp.float32),
            pltpu.VMEM((2, num_out, half, OUT_BLOCK), jnp.float32),
            pltpu.VMEM((num_out, rows, OUT_BLOCK), jnp.float32),
            pltpu.VMEM((2, half, width), jnp.float32),
            pltpu.SemaphoreType.DMA((WEIGHT_RING, 2)),
            pltpu.SemaphoreType.DMA((num_out,)),
            pltpu.SemaphoreType.DMA((5,)),
            pltpu.SemaphoreType.DMA((num_copies,)),
            pltpu.SemaphoreType.DMA((num_copies,)),
        ],
        compiler_params=pltpu.CompilerParams(collective_id=0, has_side_effects=True,
                                             vmem_limit_bytes=67043328),
        cost_estimate=pl.CostEstimate(flops=24 * rows * width * hidden,
                                      bytes_accessed=9 * width * hidden * 2,
                                      transcendentals=4 * rows * hidden),
    )(*xn_mid, *x_mid, far, w_gate, w_up, w_down)


def solution(mesh):
    row_spec = P(('dp', 'tp'), None)
    cache_spec = P(('dp', 'tp'), None, None)
    full_vec = P(None)
    full_mat = P(None, None)

    def per_device(hidden_in, k_cache, v_cache, cache_len, norm_attn, norm_mlp, w_q, w_k, w_v, w_o, w_gate, w_up, w_down):
        cos_t, sin_t = rope_tables(cache_len, w_k.shape[1])
        plan = plan_rows(cache_len)
        common = (plan, hidden_in, k_cache, v_cache, norm_mlp, w_o)
        x_first, xn_first, k_new, v_new, q_rest = attention_part(
            0, *common, proj=(norm_attn.reshape(-1, LANES), cos_t, sin_t, w_q, w_k, w_v))
        far = lax.ppermute(xn_first, 'tp', [(0, 2), (1, 3), (2, 0), (3, 1)])
        x_last, xn_last = attention_part(1, *common, q_new=(q_rest, k_new, v_new))
        hidden_out = mlp_block((xn_first, xn_last), (x_first, x_last), far, w_gate, w_up, w_down)
        return hidden_out, k_new, v_new

    return jax.shard_map(
        per_device,
        mesh=mesh,
        in_specs=(row_spec, cache_spec, cache_spec, P(('dp', 'tp')), full_vec, full_vec,
                  full_mat, full_mat, full_mat, full_mat, P(None, 'tp'), P(None, 'tp'), P('tp', None)),
        out_specs=(row_spec, row_spec, row_spec),
        check_vma=False,
    )
```
